32 devices in a mesh: seq: 16 (over z, x, core), tp: 2 (over y).
Axes of the slice: x: 2, y: 2, z: 4, core: 2. Of those that a mesh axis runs over, the one named last changes fastest.
Arguments:
- hidden_in: bfloat16 [2048, 4096], P('seq', 'tp'), may hold values from -64 to 64
- span_order: int32 [16], replicated, may hold values from 0 to 15, each once
- norm_gain: bfloat16 [4096], P('tp'), may hold values from 0.099609375 to 1.8984375
- w_query: bfloat16 [4096, 4096], P('seq', 'tp'), may hold values from -0.09375 to 0.09375
- bias_query: bfloat16 [4096], P('tp'), may hold values from -14 to 14
- key_value_weight: bfloat16 [4096, 2, 1024], P('seq', None, 'tp'), may hold values from -0.09375 to 0.09375
- bias_kv: bfloat16 [2, 1024], P(None, 'tp'), may hold values from -14 to 14
- w_out: bfloat16 [4096, 4096], P('tp', 'seq'), may hold values from -0.09375 to 0.09375
- post_gain: bfloat16 [4096], P('tp'), may hold values from 0.099609375 to 1.8984375
Outputs:
- attn_out: bfloat16 [2048, 4096], P('seq', 'tp')
- normed: bfloat16 [2048, 4096], P('seq', 'tp')
The draws below stay inside these ranges and needn't reach their ends.
Inputs may be any that keep to these rules, and one draw needn't show every extreme that they name: Each span number appears once; row r of hidden_in belongs to span span_order[r // 128].
All inputs are finite; a program needn't handle non-finite values.
Results may differ from the reference program's by a relative error of at most 0.014.
Values may be sent and summed in bfloat16 or wider, within the bound.
A program may use at most 128 MiB of HBM per device.

```python
import math
import jax
import jax.numpy as jnp
from jax import lax

MODEL_WIDTH = 4096
QUERY_HEADS = 32
KEY_VALUE_HEADS = 8
HEAD_SIZE = 128
GROUP = 4
TOK_DEV = 128
SEQ = 2048
N_SEQ = 16
N_TP = 2


def draw_hidden_in(key, part):
    base_key, column_key, row_key = jax.random.split(key, 3)
    column_ids = jnp.arange(MODEL_WIDTH, dtype=jnp.float32) / MODEL_WIDTH
    base = jnp.clip(jax.random.normal(base_key, (SEQ, MODEL_WIDTH), jnp.float32), -4.0, 4.0)
    ramp = jnp.exp(0.5 * math.log(3.0) * column_ids)
    ramp = ramp / jnp.mean(ramp)
    columns = jnp.exp(jax.random.uniform(column_key, (MODEL_WIDTH,), jnp.float32, -1.1513, 1.1513))
    rows = jnp.exp(jax.random.uniform(row_key, (SEQ, 1), jnp.float32, -1.1513, 1.1513))
    field = jnp.clip(base * rows * (columns * ramp)[None, :], -64.0, 64.0)
    return field.astype(jnp.bfloat16)


def draw_bias_query(key, part):
    random_jitter = jax.random.normal(jax.random.fold_in(key, 11), (QUERY_HEADS * HEAD_SIZE,), jnp.float32)
    return jnp.clip(0.5 * random_jitter, -2.0, 2.0).astype(jnp.bfloat16)


def draw_bias_kv(key, part):
    random_jitter = jax.random.normal(jax.random.fold_in(key, 13), (2, KEY_VALUE_HEADS * HEAD_SIZE), jnp.float32)
    return jnp.clip(0.5 * random_jitter, -2.0, 2.0).astype(jnp.bfloat16)


def steps_of(stream_key, extent, pieces, low, top_value):
    factor_of = 1.0
    for position, shards_of in pieces:
        heights = jax.random.uniform(jax.random.fold_in(jax.random.fold_in(stream_key, 6), position), (shards_of,), jnp.float32, low / len(pieces), top_value / len(pieces))
        factor_of = factor_of * jnp.repeat(jnp.exp(heights), extent[position] // shards_of).reshape((-1,) + (1,) * (len(extent) - 1 - position))
    return factor_of


def noise(rng, dims, deviation, most, cuts=(), held_as=jnp.bfloat16):
    factor_of = steps_of(rng, dims, cuts, -0.22, 0.18) if cuts else 1.0
    result = jax.random.normal(rng, dims, jnp.float32) * deviation * factor_of
    return jnp.minimum(jnp.maximum(result, -most), most).astype(held_as)


def setup_inputs(seed: int = 0) -> dict:
    arg_keys = jax.random.split(jax.random.key(seed), 10)
    hidden_in = draw_hidden_in(jax.random.fold_in(arg_keys[9], 71), 0)
    span_order = jax.random.permutation(arg_keys[1], N_SEQ).astype(jnp.int32)
    norm_gain = jnp.clip(1.0 + 0.18 * jax.random.normal(arg_keys[2], (MODEL_WIDTH,), jnp.float32), 0.099609375, 1.8984375).astype(jnp.bfloat16)
    w_query = noise(arg_keys[3], (MODEL_WIDTH, QUERY_HEADS * HEAD_SIZE), MODEL_WIDTH ** -0.5, 0.09375, ((0, 16), (1, 2)))
    bias_query = draw_bias_query(jax.random.fold_in(arg_keys[9], 71), 0)
    key_value_weight = noise(arg_keys[5], (MODEL_WIDTH, 2, KEY_VALUE_HEADS * HEAD_SIZE), MODEL_WIDTH ** -0.5, 0.09375, ((0, 16), (2, 2)))
    bias_kv = draw_bias_kv(jax.random.fold_in(arg_keys[9], 71), 0)
    w_out = noise(arg_keys[7], (QUERY_HEADS * HEAD_SIZE, MODEL_WIDTH), (QUERY_HEADS * HEAD_SIZE) ** -0.5, 0.09375, ((0, 2), (1, 16)))
    post_gain = jnp.clip(1.0 + 0.18 * jax.random.normal(arg_keys[8], (MODEL_WIDTH,), jnp.float32), 0.099609375, 1.8984375).astype(jnp.bfloat16)
    return dict(hidden_in=hidden_in, span_order=span_order, norm_gain=norm_gain, w_query=w_query, bias_query=bias_query, key_value_weight=key_value_weight, bias_kv=bias_kv, w_out=w_out, post_gain=post_gain)


eps = 1e-06
rope_base = 1000000.0

def apply_rotary(field, token_positions):
    half = field.shape[-1] // 2
    inverse = jnp.exp(-math.log(rope_base) * jnp.arange(half, dtype=jnp.float32) / half)
    angles = token_positions.astype(jnp.float32)[:, None] * inverse[None, :]
    cosine = jnp.cos(angles)[:, None, :]
    sine = jnp.sin(angles)[:, None, :]
    first = field[..., :half]
    second = field[..., half:]
    return jnp.concatenate([first * cosine - second * sine, second * cosine + first * sine], axis=-1)

def reference(hidden_in, span_order, norm_gain, w_query, bias_query, key_value_weight, bias_kv, w_out, post_gain):
    sequence_length = hidden_in.shape[0]
    row_ids = jnp.arange(sequence_length, dtype=jnp.int32)
    token_positions = (span_order[row_ids // TOK_DEV] * TOK_DEV + row_ids % TOK_DEV).astype(jnp.int32)
    local = hidden_in.astype(jnp.float32)
    meansq = lax.optimization_barrier(jnp.mean(local * local, axis=1, keepdims=True))
    normed_in = (local * lax.rsqrt(meansq + eps) * norm_gain.astype(jnp.float32)[None, :]).astype(jnp.bfloat16)
    query_proj = jnp.dot(normed_in, w_query, preferred_element_type=jnp.float32) + bias_query.astype(jnp.float32)[None, :]
    queries = apply_rotary(query_proj.reshape(sequence_length, QUERY_HEADS, HEAD_SIZE), token_positions).astype(jnp.bfloat16)
    key_projected = jnp.dot(normed_in, key_value_weight[:, 0, :], preferred_element_type=jnp.float32) + bias_kv[0].astype(jnp.float32)[None, :]
    value_projected = jnp.dot(normed_in, key_value_weight[:, 1, :], preferred_element_type=jnp.float32) + bias_kv[1].astype(jnp.float32)[None, :]
    rotated_keys = apply_rotary(key_projected.reshape(sequence_length, KEY_VALUE_HEADS, HEAD_SIZE), token_positions).astype(jnp.bfloat16)
    value_rows = value_projected.astype(jnp.bfloat16).reshape(sequence_length, KEY_VALUE_HEADS, HEAD_SIZE)
    query_major = queries.transpose(1, 0, 2)
    key_major = jnp.repeat(rotated_keys.transpose(1, 0, 2), GROUP, axis=0)
    value_major = jnp.repeat(value_rows.transpose(1, 0, 2), GROUP, axis=0)
    allowed = token_positions[None, :] <= token_positions[:, None]
    scale = 1.0 / math.sqrt(HEAD_SIZE)

    def one_head(triple):
        query_one, key_one, value_one = triple
        scores = jnp.dot(query_one, key_one.T, preferred_element_type=jnp.float32) * scale
        scores = jnp.where(allowed, scores, -jnp.inf)
        peak = lax.optimization_barrier(jnp.max(scores, axis=1, keepdims=True))
        weights = jnp.where(allowed, jnp.exp(scores - peak), 0.0)
        totals = lax.optimization_barrier(jnp.sum(weights, axis=1, keepdims=True))
        summed = jnp.dot(weights.astype(jnp.bfloat16), value_one, preferred_element_type=jnp.float32)
        return (summed / totals).astype(jnp.bfloat16)
    attended = lax.map(one_head, (query_major, key_major, value_major))
    attended = attended.transpose(1, 0, 2).reshape(sequence_length, QUERY_HEADS * HEAD_SIZE)
    part_rows = QUERY_HEADS * HEAD_SIZE // N_TP
    mixed = jnp.zeros((sequence_length, MODEL_WIDTH), jnp.float32)
    for group in range(N_TP):
        lower = group * part_rows
        piece = jnp.dot(attended[:, lower:lower + part_rows], w_out[lower:lower + part_rows, :], preferred_element_type=jnp.float32)
        mixed = mixed + lax.optimization_barrier(piece.astype(jnp.bfloat16)).astype(jnp.float32)
    attn_out = mixed.astype(jnp.bfloat16)
    stream = local + mixed
    post_sq = lax.optimization_barrier(jnp.mean(stream * stream, axis=1, keepdims=True))
    normed = (stream * lax.rsqrt(post_sq + eps) * post_gain.astype(jnp.float32)[None, :]).astype(jnp.bfloat16)
    return (attn_out, normed)
```

```python
import math

import jax
import jax.numpy as jnp
from jax import lax
from jax.experimental import pallas as pl
from jax.experimental.pallas import tpu as pltpu
from jax.sharding import PartitionSpec as P

MODEL_WIDTH = 4096
HEAD_SIZE = 128
GROUP = 4


eps = 1e-06
rope_base = 1000000.0


def apply_rotary(field, token_positions):
    half = field.shape[-1] // 2
    inverse = jnp.exp(-math.log(rope_base) * jnp.arange(half, dtype=jnp.float32) / half)
    angles = token_positions.astype(jnp.float32)[:, None] * inverse[None, :]
    cosine = jnp.cos(angles)[:, None, :]
    sine = jnp.sin(angles)[:, None, :]
    first = field[..., :half]
    second = field[..., half:]
    return jnp.concatenate(
        [first * cosine - second * sine, second * cosine + first * sine], axis=-1
    )


def span_lookup(order, devices):
    table_ids = jnp.arange(order.shape[0], dtype=jnp.int32)
    return jnp.sum(jnp.where(devices[:, None] == table_ids[None, :], order[None, :], 0), axis=1)


def per_device_by_span(
    hidden_in,
    span_order,
    norm_gain,
    w_query,
    bias_query,
    key_value_weight,
    bias_kv,
    w_out,
    post_gain,
):
    tok_rows = hidden_in.shape[0]
    seq_index = lax.axis_index("seq")
    own_span = span_lookup(span_order, jnp.full((1,), seq_index, jnp.int32))[0]
    token_positions = own_span * tok_rows + jnp.arange(tok_rows, dtype=jnp.int32)
    local = hidden_in.astype(jnp.float32)
    raw_rows, gains = (
        lax.all_gather(hidden_in, "tp", axis=1, tiled=True),
        lax.all_gather(norm_gain[None, :], "tp", axis=1, tiled=True),
    )
    full_rows = raw_rows.astype(jnp.float32)
    meansq = jnp.mean(full_rows * full_rows, axis=1, keepdims=True)
    normed_in = (full_rows * lax.rsqrt(meansq + eps) * gains.astype(jnp.float32)).astype(
        jnp.bfloat16
    )
    columns = normed_in
    query_proj = jnp.dot(
        columns,
        lax.all_gather(w_query, "seq", axis=0, tiled=True),
        preferred_element_type=jnp.float32,
    )
    columns = normed_in
    pair_proj = jnp.einsum(
        "tr,rkc->tkc",
        columns,
        lax.all_gather(key_value_weight, "seq", axis=0, tiled=True),
        preferred_element_type=jnp.float32,
    )
    query_heads = w_query.shape[1] // HEAD_SIZE
    kv_heads = key_value_weight.shape[2] // HEAD_SIZE
    query_proj = query_proj + bias_query.astype(jnp.float32)[None, :]
    queries = apply_rotary(
        query_proj.reshape(tok_rows, query_heads, HEAD_SIZE), token_positions
    ).astype(jnp.bfloat16)
    pair_proj = pair_proj + bias_kv.astype(jnp.float32)[None, :, :]
    rotated_keys = apply_rotary(
        pair_proj[:, 0, :].reshape(tok_rows, kv_heads, HEAD_SIZE), token_positions
    )
    rotated_keys = rotated_keys.astype(jnp.bfloat16).reshape(tok_rows, kv_heads * HEAD_SIZE)
    value_rows = pair_proj[:, 1, :].astype(jnp.bfloat16)
    grouped = (
        queries.reshape(tok_rows, kv_heads, GROUP, HEAD_SIZE)
        .transpose(1, 2, 0, 3)
        .reshape(kv_heads, GROUP * tok_rows, HEAD_SIZE)
    )
    query_pos = jnp.tile(token_positions, GROUP)
    last_query = jnp.max(token_positions)
    scale = 1.0 / math.sqrt(HEAD_SIZE)
    start_state = (
        jnp.full((kv_heads, GROUP * tok_rows), -1e30, jnp.float32),
        jnp.zeros((kv_heads, GROUP * tok_rows), jnp.float32),
        jnp.zeros((kv_heads, GROUP * tok_rows, HEAD_SIZE), jnp.float32),
    )
    key_piece = lax.all_gather(rotated_keys, "seq", axis=0, tiled=True)
    value_piece = lax.all_gather(value_rows, "seq", axis=0, tiled=True)
    count = key_piece.shape[0]
    block = math.gcd(count, 1536)

    def visit(step, state):
        first = step * block
        key_block = lax.dynamic_slice_in_dim(key_piece, first, block, 0).reshape(
            block, kv_heads, HEAD_SIZE
        )
        value_block = lax.dynamic_slice_in_dim(value_piece, first, block, 0).reshape(
            block, kv_heads, HEAD_SIZE
        )
        row_ids = first + jnp.arange(block, dtype=jnp.int32)
        key_pos = span_lookup(span_order, row_ids // tok_rows) * tok_rows + row_ids % tok_rows

        def update(current):
            maxima, totals, sums = current
            scores = (
                jnp.einsum("kqd,nkd->kqn", grouped, key_block, preferred_element_type=jnp.float32)
                * scale
            )
            allowed = (key_pos[None, :] <= query_pos[:, None])[None, :, :]
            scores = jnp.where(allowed, scores, -1e30)
            fresh = jnp.maximum(maxima, jnp.max(scores, axis=2))
            weights = jnp.where(allowed, jnp.exp(scores - fresh[:, :, None]), 0.0)
            factor = jnp.exp(maxima - fresh)
            totals = totals * factor + jnp.sum(weights, axis=2)
            sums = sums * factor[:, :, None] + jnp.einsum(
                "kqn,nkd->kqd",
                weights.astype(jnp.bfloat16),
                value_block,
                preferred_element_type=jnp.float32,
            )
            return (fresh, totals, sums)

        return lax.cond(jnp.min(key_pos) <= last_query, update, lambda current: current, state)

    maxima, totals, sums = lax.fori_loop(0, count // block, visit, start_state)
    attended = (sums / totals[:, :, None]).astype(jnp.bfloat16)
    attended = (
        attended.reshape(kv_heads, GROUP, tok_rows, HEAD_SIZE)
        .transpose(2, 0, 1, 3)
        .reshape(tok_rows, query_heads * HEAD_SIZE)
    )
    partial_out = jnp.dot(
        attended,
        lax.all_gather(w_out, "seq", axis=1, tiled=True),
        preferred_element_type=jnp.float32,
    )
    mixed = lax.psum_scatter(
        partial_out.astype(jnp.bfloat16), "tp", scatter_dimension=1, tiled=True
    ).astype(jnp.float32)
    attn_out = mixed.astype(jnp.bfloat16)
    stream = local + mixed
    post_sq = lax.psum(jnp.sum(stream * stream, axis=1), "tp")
    normed = (
        stream
        * lax.rsqrt(post_sq / MODEL_WIDTH + eps)[:, None]
        * post_gain.astype(jnp.float32)[None, :]
    ).astype(jnp.bfloat16)
    return (attn_out, normed)


def rope_tables(span_order, tok_rows):
    half = HEAD_SIZE // 2
    rows = (span_order[:, None] * tok_rows + jnp.arange(tok_rows, dtype=jnp.int32)[None, :]).reshape(-1)
    inverse = jnp.exp(-math.log(rope_base) * jnp.arange(half, dtype=jnp.float32) / half)
    angles = rows.astype(jnp.float32)[:, None] * inverse[None, :]
    cosine, sine = jnp.cos(angles), jnp.sin(angles)
    return (
        rows,
        jnp.concatenate([cosine, cosine], axis=1),
        jnp.concatenate([-sine, sine], axis=1),
    )


def attention_kernel(q_ref, k_ref, v_ref, qpos_ref, kpos_ref, out_ref):
    scores = lax.dot_general(
        q_ref[...], k_ref[...], (((1,), (1,)), ((), ())), preferred_element_type=jnp.float32
    ) * (1.0 / math.sqrt(HEAD_SIZE))
    allowed = kpos_ref[...] <= qpos_ref[...]
    scores = jnp.where(allowed, scores, -jnp.inf)
    peak = jnp.max(scores, axis=1, keepdims=True)
    weights = jnp.exp(scores - peak)
    totals = jnp.sum(weights, axis=1, keepdims=True)
    summed = jnp.dot(
        weights.astype(jnp.bfloat16), v_ref[...], preferred_element_type=jnp.float32
    )
    out_ref[...] = (summed / totals).astype(jnp.bfloat16)


def attention(queries, keys, values, positions):
    count = queries.shape[0]
    block = math.gcd(count, 256)
    rows = pl.BlockSpec((block, HEAD_SIZE), lambda i: (i, 0))
    whole = pl.BlockSpec((count, HEAD_SIZE), lambda i: (0, 0))
    return pl.pallas_call(
        attention_kernel,
        grid=(count // block,),
        in_specs=[
            rows,
            whole,
            whole,
            pl.BlockSpec((block, 1), lambda i: (i, 0)),
            pl.BlockSpec((1, count), lambda i: (0, 0)),
        ],
        out_specs=rows,
        out_shape=jax.ShapeDtypeStruct((count, HEAD_SIZE), jnp.bfloat16),
        cost_estimate=pl.CostEstimate(
            flops=4 * count * count * HEAD_SIZE,
            bytes_accessed=8 * count * HEAD_SIZE,
            transcendentals=count * count,
        ),
        name="attention",
    )(queries, keys, values, positions[:, None], positions[None, :])


def per_device_by_head(
    hidden_in,
    span_order,
    norm_gain,
    w_query,
    bias_query,
    key_value_weight,
    bias_kv,
    w_out,
    post_gain,
):
    tok_rows, width = hidden_in.shape
    n_seq = span_order.shape[0]
    n_tp = MODEL_WIDTH // width
    me = lax.axis_index("seq")
    slab = w_query.shape[0]
    kv_heads = key_value_weight.shape[2] // HEAD_SIZE
    share = n_seq // kv_heads
    pieces = jnp.concatenate(
        [
            w_query.reshape(slab, n_seq, 1, HEAD_SIZE),
            jnp.repeat(
                key_value_weight.reshape(slab, 2, kv_heads, HEAD_SIZE).transpose(0, 2, 1, 3),
                share,
                axis=1,
            ),
        ],
        axis=2,
    ).transpose(1, 0, 2, 3).reshape(n_seq, slab, 3 * HEAD_SIZE)
    weights = lax.all_to_all(pieces, "seq", split_axis=0, concat_axis=0, tiled=True)
    weights = weights.reshape(n_tp, width, 3 * HEAD_SIZE)
    local = hidden_in.astype(jnp.float32)
    meansq = lax.psum(jnp.sum(local * local, axis=1, keepdims=True), "tp") / MODEL_WIDTH
    normed_in = (
        local * lax.rsqrt(meansq + eps) * norm_gain.astype(jnp.float32)[None, :]
    ).astype(jnp.bfloat16)
    everyone = lax.all_gather(normed_in, ("seq", "tp")).reshape(n_seq, n_tp, tok_rows, width)
    tokens = n_seq * tok_rows
    proj = jnp.einsum("stpr,trc->spc", everyone, weights, preferred_element_type=jnp.float32)
    proj = proj.reshape(tokens, 3 * HEAD_SIZE)
    bias_q = lax.dynamic_slice_in_dim(bias_query, me * HEAD_SIZE, HEAD_SIZE)
    bias_pair = lax.dynamic_slice_in_dim(bias_kv, me // share * HEAD_SIZE, HEAD_SIZE, 1)
    bias = jnp.concatenate([bias_q, bias_pair[0], bias_pair[1]]).astype(jnp.float32)
    proj = proj + bias[None, :]
    positions, cosine, sine = rope_tables(span_order, tok_rows)

    def rotated(field):
        return (field * cosine + jnp.roll(field, HEAD_SIZE // 2, axis=1) * sine).astype(jnp.bfloat16)

    queries = rotated(proj[:, :HEAD_SIZE])
    keys = rotated(proj[:, HEAD_SIZE : 2 * HEAD_SIZE])
    values = proj[:, 2 * HEAD_SIZE :].astype(jnp.bfloat16)
    attended = attention(queries, keys, values, positions)
    heads = lax.all_gather(attended, "seq")
    columns = w_out.shape[1]
    partial_out = jnp.einsum(
        "htd,hdc->tc",
        heads,
        w_out.reshape(n_seq, HEAD_SIZE, columns),
        preferred_element_type=jnp.float32,
    ).astype(jnp.bfloat16)
    blocks = lax.all_to_all(
        partial_out.reshape(n_seq, tok_rows, columns), "seq", split_axis=0, concat_axis=0, tiled=True
    )
    blocks = blocks.reshape(n_tp, n_seq // n_tp, tok_rows, columns)
    terms = lax.all_to_all(blocks, "tp", split_axis=0, concat_axis=0, tiled=True)
    mixed = jnp.sum(terms.astype(jnp.float32), axis=0).transpose(1, 0, 2).reshape(tok_rows, width)
    attn_out = mixed.astype(jnp.bfloat16)
    stream = local + mixed
    post_sq = lax.psum(jnp.sum(stream * stream, axis=1), "tp")
    normed = (
        stream
        * lax.rsqrt(post_sq / MODEL_WIDTH + eps)[:, None]
        * post_gain.astype(jnp.float32)[None, :]
    ).astype(jnp.bfloat16)
    return (attn_out, normed)


def per_device(*args):
    hidden_in, span_order, w_query, kv_weight = args[0], args[1], args[3], args[5]
    n_seq = span_order.shape[0]
    n_tp = MODEL_WIDTH // hidden_in.shape[1]
    heads = w_query.shape[1] // HEAD_SIZE
    kv_heads = kv_weight.shape[2] // HEAD_SIZE
    if heads == n_seq and n_seq == kv_heads * GROUP and n_seq % n_tp == 0:
        return per_device_by_head(*args)
    return per_device_by_span(*args)


def solution(mesh):
    placed = (
        P("seq", "tp"),
        P(),
        P("tp"),
        P("seq", "tp"),
        P("tp"),
        P("seq", None, "tp"),
        P(None, "tp"),
        P("tp", "seq"),
        P("tp"),
    )
    return jax.shard_map(
        per_device,
        mesh=mesh,
        in_specs=placed,
        out_specs=(P("seq", "tp"), P("seq", "tp")),
        check_vma=False,
    )
```

```python
import math

import jax
import jax.numpy as jnp
from jax import lax
from jax.experimental import pallas as pl
from jax.experimental.pallas import tpu as pltpu
from jax.sharding import PartitionSpec as P

MODEL_WIDTH = 4096
HEAD_SIZE = 128
GROUP = 4


eps = 1e-06
rope_base = 1000000.0


def apply_rotary(field, token_positions):
    half = field.shape[-1] // 2
    inverse = jnp.exp(-math.log(rope_base) * jnp.arange(half, dtype=jnp.float32) / half)
    angles = token_positions.astype(jnp.float32)[:, None] * inverse[None, :]
    cosine = jnp.cos(angles)[:, None, :]
    sine = jnp.sin(angles)[:, None, :]
    first = field[..., :half]
    second = field[..., half:]
    return jnp.concatenate(
        [first * cosine - second * sine, second * cosine + first * sine], axis=-1
    )


def span_lookup(order, devices):
    table_ids = jnp.arange(order.shape[0], dtype=jnp.int32)
    return jnp.sum(jnp.where(devices[:, None] == table_ids[None, :], order[None, :], 0), axis=1)


def per_device_by_span(
    hidden_in,
    span_order,
    norm_gain,
    w_query,
    bias_query,
    key_value_weight,
    bias_kv,
    w_out,
    post_gain,
):
    tok_rows = hidden_in.shape[0]
    seq_index = lax.axis_index("seq")
    own_span = span_lookup(span_order, jnp.full((1,), seq_index, jnp.int32))[0]
    token_positions = own_span * tok_rows + jnp.arange(tok_rows, dtype=jnp.int32)
    local = hidden_in.astype(jnp.float32)
    raw_rows, gains = (
        lax.all_gather(hidden_in, "tp", axis=1, tiled=True),
        lax.all_gather(norm_gain[None, :], "tp", axis=1, tiled=True),
    )
    full_rows = raw_rows.astype(jnp.float32)
    meansq = jnp.mean(full_rows * full_rows, axis=1, keepdims=True)
    normed_in = (full_rows * lax.rsqrt(meansq + eps) * gains.astype(jnp.float32)).astype(
        jnp.bfloat16
    )
    columns = normed_in
    query_proj = jnp.dot(
        columns,
        lax.all_gather(w_query, "seq", axis=0, tiled=True),
        preferred_element_type=jnp.float32,
    )
    columns = normed_in
    pair_proj = jnp.einsum(
        "tr,rkc->tkc",
        columns,
        lax.all_gather(key_value_weight, "seq", axis=0, tiled=True),
        preferred_element_type=jnp.float32,
    )
    query_heads = w_query.shape[1] // HEAD_SIZE
    kv_heads = key_value_weight.shape[2] // HEAD_SIZE
    query_proj = query_proj + bias_query.astype(jnp.float32)[None, :]
    queries = apply_rotary(
        query_proj.reshape(tok_rows, query_heads, HEAD_SIZE), token_positions
    ).astype(jnp.bfloat16)
    pair_proj = pair_proj + bias_kv.astype(jnp.float32)[None, :, :]
    rotated_keys = apply_rotary(
        pair_proj[:, 0, :].reshape(tok_rows, kv_heads, HEAD_SIZE), token_positions
    )
    rotated_keys = rotated_keys.astype(jnp.bfloat16).reshape(tok_rows, kv_heads * HEAD_SIZE)
    value_rows = pair_proj[:, 1, :].astype(jnp.bfloat16)
    grouped = (
        queries.reshape(tok_rows, kv_heads, GROUP, HEAD_SIZE)
        .transpose(1, 2, 0, 3)
        .reshape(kv_heads, GROUP * tok_rows, HEAD_SIZE)
    )
    query_pos = jnp.tile(token_positions, GROUP)
    last_query = jnp.max(token_positions)
    scale = 1.0 / math.sqrt(HEAD_SIZE)
    start_state = (
        jnp.full((kv_heads, GROUP * tok_rows), -1e30, jnp.float32),
        jnp.zeros((kv_heads, GROUP * tok_rows), jnp.float32),
        jnp.zeros((kv_heads, GROUP * tok_rows, HEAD_SIZE), jnp.float32),
    )
    key_piece = lax.all_gather(rotated_keys, "seq", axis=0, tiled=True)
    value_piece = lax.all_gather(value_rows, "seq", axis=0, tiled=True)
    count = key_piece.shape[0]
    block = math.gcd(count, 1536)

    def visit(step, state):
        first = step * block
        key_block = lax.dynamic_slice_in_dim(key_piece, first, block, 0).reshape(
            block, kv_heads, HEAD_SIZE
        )
        value_block = lax.dynamic_slice_in_dim(value_piece, first, block, 0).reshape(
            block, kv_heads, HEAD_SIZE
        )
        row_ids = first + jnp.arange(block, dtype=jnp.int32)
        key_pos = span_lookup(span_order, row_ids // tok_rows) * tok_rows + row_ids % tok_rows

        def update(current):
            maxima, totals, sums = current
            scores = (
                jnp.einsum("kqd,nkd->kqn", grouped, key_block, preferred_element_type=jnp.float32)
                * scale
            )
            allowed = (key_pos[None, :] <= query_pos[:, None])[None, :, :]
            scores = jnp.where(allowed, scores, -1e30)
            fresh = jnp.maximum(maxima, jnp.max(scores, axis=2))
            weights = jnp.where(allowed, jnp.exp(scores - fresh[:, :, None]), 0.0)
            factor = jnp.exp(maxima - fresh)
            totals = totals * factor + jnp.sum(weights, axis=2)
            sums = sums * factor[:, :, None] + jnp.einsum(
                "kqn,nkd->kqd",
                weights.astype(jnp.bfloat16),
                value_block,
                preferred_element_type=jnp.float32,
            )
            return (fresh, totals, sums)

        return lax.cond(jnp.min(key_pos) <= last_query, update, lambda current: current, state)

    maxima, totals, sums = lax.fori_loop(0, count // block, visit, start_state)
    attended = (sums / totals[:, :, None]).astype(jnp.bfloat16)
    attended = (
        attended.reshape(kv_heads, GROUP, tok_rows, HEAD_SIZE)
        .transpose(2, 0, 1, 3)
        .reshape(tok_rows, query_heads * HEAD_SIZE)
    )
    partial_out = jnp.dot(
        attended,
        lax.all_gather(w_out, "seq", axis=1, tiled=True),
        preferred_element_type=jnp.float32,
    )
    mixed = lax.psum_scatter(
        partial_out.astype(jnp.bfloat16), "tp", scatter_dimension=1, tiled=True
    ).astype(jnp.float32)
    attn_out = mixed.astype(jnp.bfloat16)
    stream = local + mixed
    post_sq = lax.psum(jnp.sum(stream * stream, axis=1), "tp")
    normed = (
        stream
        * lax.rsqrt(post_sq / MODEL_WIDTH + eps)[:, None]
        * post_gain.astype(jnp.float32)[None, :]
    ).astype(jnp.bfloat16)
    return (attn_out, normed)


def rope_tables(span_order, tok_rows):
    half = HEAD_SIZE // 2
    rows = (span_order[:, None] * tok_rows + jnp.arange(tok_rows, dtype=jnp.int32)[None, :]).reshape(-1)
    inverse = jnp.exp(-math.log(rope_base) * jnp.arange(half, dtype=jnp.float32) / half)
    angles = rows.astype(jnp.float32)[:, None] * inverse[None, :]
    cosine, sine = jnp.cos(angles), jnp.sin(angles)
    return (
        rows,
        jnp.concatenate([cosine, cosine], axis=1),
        jnp.concatenate([-sine, sine], axis=1),
    )


def attention_kernel(q_ref, k_ref, v_ref, qpos_ref, kpos_ref, out_ref):
    scores = lax.dot_general(
        q_ref[...], k_ref[...], (((1,), (1,)), ((), ())), preferred_element_type=jnp.float32
    ) * (1.0 / math.sqrt(HEAD_SIZE))
    allowed = kpos_ref[...] <= qpos_ref[...]
    scores = jnp.where(allowed, scores, -jnp.inf)
    peak = jnp.max(scores, axis=1, keepdims=True)
    weights = jnp.exp(scores - peak)
    totals = jnp.sum(weights, axis=1, keepdims=True)
    summed = jnp.dot(
        weights.astype(jnp.bfloat16), v_ref[...], preferred_element_type=jnp.float32
    )
    out_ref[...] = (summed / totals).astype(jnp.bfloat16)


def attention(queries, keys, values, positions):
    count = queries.shape[0]
    block = math.gcd(count, 256)
    rows = pl.BlockSpec((block, HEAD_SIZE), lambda i: (i, 0))
    whole = pl.BlockSpec((count, HEAD_SIZE), lambda i: (0, 0))
    return pl.pallas_call(
        attention_kernel,
        grid=(count // block,),
        in_specs=[
            rows,
            whole,
            whole,
            pl.BlockSpec((block, 1), lambda i: (i, 0)),
            pl.BlockSpec((1, count), lambda i: (0, 0)),
        ],
        out_specs=rows,
        out_shape=jax.ShapeDtypeStruct((count, HEAD_SIZE), jnp.bfloat16),
        cost_estimate=pl.CostEstimate(
            flops=4 * count * count * HEAD_SIZE,
            bytes_accessed=8 * count * HEAD_SIZE,
            transcendentals=count * count,
        ),
        name="attention",
    )(queries, keys, values, positions[:, None], positions[None, :])


MESH = pl.DeviceIdType.MESH
CORES = 2
PLANE = 4


class Traffic:
    def __init__(self, send_sem, peer):
        self.send_sem, self.peer, self.started = send_sem, peer, []

    def send(self, source, landing, arrival, target):
        copy = pltpu.make_async_remote_copy(
            src_ref=source,
            dst_ref=landing,
            send_sem=self.send_sem.at[len(self.started)],
            recv_sem=arrival,
            device_id=target,
            device_id_type=MESH,
        )
        copy.start()
        self.started.append(copy)

    def arrive(self, landing, arrival):
        pltpu.make_async_remote_copy(
            src_ref=landing,
            dst_ref=landing,
            send_sem=self.send_sem.at[0],
            recv_sem=arrival,
            device_id=self.peer,
            device_id_type=MESH,
        ).wait_recv()

    def finish(self):
        for copy in self.started:
            copy.wait_send()


def place(n_seq):
    s, t = lax.axis_index("seq"), lax.axis_index("tp")
    return s, t, s // PLANE, s % PLANE // CORES, s % CORES


def at(z, x, c):
    return z * PLANE + x * CORES + c


def exchange_kernel(
    n_seq, chunk, q_in, kv_in, rows_out, q_out, kv_out, local_sem, send_sem, rows_sem, q_sem, kv_sem
):
    s, t, z, x, c = place(n_seq)
    depth = n_seq // PLANE
    offset = s % PLANE
    sibling, across = (at(z, x, 1 - c), t), (at(z, 1 - x, c), t)
    other = (s, 1 - t)
    go = Traffic(send_sem, sibling)
    stay = [
        pltpu.make_async_copy(chunk, rows_out.at[s, t], local_sem.at[0]),
        pltpu.make_async_copy(q_in.at[s], q_out.at[s], local_sem.at[1]),
        pltpu.make_async_copy(kv_in.at[z], kv_out.at[s], local_sem.at[2]),
    ]
    for copy in stay:
        copy.start()

    def pass_on(source, owner, part, targets):
        for target in targets:
            go.send(source, rows_out.at[owner, part], rows_sem.at[owner, part], target)

    def await_rows(owner, part):
        go.arrive(rows_out.at[owner, part], rows_sem.at[owner, part])

    far = [lax.rem(z + d, depth) for d in range(1, depth)]
    near = [lax.rem(z - d + depth, depth) for d in range(depth)]
    pass_on(chunk, s, t, [other, across])
    pass_on(chunk, s, t, [(at(zt, x, c), t) for zt in far])
    pass_on(chunk, s, t, [sibling])
    for zt in far:
        target = at(zt, x, c)
        go.send(kv_in.at[zt], kv_out.at[s], kv_sem.at[s], (target, t))
    mates = [lax.rem(offset + r, PLANE) for r in range(1, PLANE)]
    for mate in mates:
        go.send(kv_in.at[z], kv_out.at[s], kv_sem.at[s], (z * PLANE + mate, t))
    for d in range(1, n_seq):
        target = lax.rem(s + d, n_seq)
        go.send(q_in.at[target], q_out.at[s], q_sem.at[s], (target, t))
    for zs in near[1:]:
        owner = at(zs, x, c)
        await_rows(owner, t)
        pass_on(rows_out.at[owner, t], owner, t, [other, across, sibling])
    for zs in near:
        owner = at(zs, 1 - x, c)
        await_rows(owner, t)
        pass_on(rows_out.at[owner, t], owner, t, [other, sibling])
    for zs in near[1:]:
        owner = at(zs, x, c)
        go.arrive(kv_out.at[owner], kv_sem.at[owner])
        for mate in mates:
            go.send(kv_out.at[owner], kv_out.at[owner], kv_sem.at[owner], (z * PLANE + mate, t))
    for xs in (x, 1 - x):
        for zs in near:
            owner = at(zs, xs, c)
            await_rows(owner, 1 - t)
            pass_on(rows_out.at[owner, 1 - t], owner, 1 - t, [sibling])
    for part in (t, 1 - t):
        for xs in (x, 1 - x):
            for zs in near:
                await_rows(at(zs, xs, 1 - c), part)
    for d in range(1, n_seq):
        owner = lax.rem(s - d + n_seq, n_seq)
        go.arrive(q_out.at[owner], q_sem.at[owner])
    for mate in mates:
        for zs in near:
            owner = zs * PLANE + mate
            go.arrive(kv_out.at[owner], kv_sem.at[owner])
    for copy in stay:
        copy.wait()
    go.finish()


def exchange(chunk, q_pieces, kv_pieces, n_seq, n_tp):
    vmem = pl.BlockSpec(memory_space=pltpu.VMEM)
    hbm = pl.BlockSpec(memory_space=pl.ANY)
    dma = pltpu.SemaphoreType.DMA
    return pl.pallas_call(
        lambda *refs: exchange_kernel(n_seq, *refs),
        out_shape=(
            jax.ShapeDtypeStruct((n_seq, n_tp) + chunk.shape, chunk.dtype),
            jax.ShapeDtypeStruct(q_pieces.shape, q_pieces.dtype),
            jax.ShapeDtypeStruct((n_seq,) + kv_pieces.shape[1:], kv_pieces.dtype),
        ),
        in_specs=[vmem] * 3,
        out_specs=(hbm,) * 3,
        scratch_shapes=[
            dma((3,)),
            dma((6 * n_seq,)),
            dma((n_seq, n_tp)),
            dma((n_seq,)),
            dma((n_seq,)),
        ],
        compiler_params=pltpu.CompilerParams(has_side_effects=True),
        name="exchange",
    )(chunk, q_pieces, kv_pieces)


def heads_kernel(n_seq, chunk, heads_out, local_sem, send_sem, heads_sem):
    s, t, z, x, c = place(n_seq)
    depth = n_seq // PLANE
    sibling, across = (at(z, x, 1 - c), t), (at(z, 1 - x, c), t)
    go = Traffic(send_sem, sibling)
    stay = pltpu.make_async_copy(chunk, heads_out.at[s], local_sem.at[0])
    stay.start()
    near = [lax.rem(z - d + depth, depth) for d in range(depth)]
    targets = [across] + [(at(lax.rem(z + d, depth), x, c), t) for d in range(1, depth)] + [sibling]
    for target in targets:
        go.send(chunk, heads_out.at[s], heads_sem.at[s], target)
    for zs in near[1:]:
        owner = at(zs, x, c)
        go.arrive(heads_out.at[owner], heads_sem.at[owner])
        for target in (across, sibling):
            go.send(heads_out.at[owner], heads_out.at[owner], heads_sem.at[owner], target)
    for zs in near:
        owner = at(zs, 1 - x, c)
        go.arrive(heads_out.at[owner], heads_sem.at[owner])
        go.send(heads_out.at[owner], heads_out.at[owner], heads_sem.at[owner], sibling)
    for xs in (x, 1 - x):
        for zs in near:
            owner = at(zs, xs, 1 - c)
            go.arrive(heads_out.at[owner], heads_sem.at[owner])
    stay.wait()
    go.finish()


def gather_heads(chunk, n_seq):
    dma = pltpu.SemaphoreType.DMA
    return pl.pallas_call(
        lambda *refs: heads_kernel(n_seq, *refs),
        out_shape=jax.ShapeDtypeStruct((n_seq,) + chunk.shape, chunk.dtype),
        in_specs=[pl.BlockSpec(memory_space=pltpu.VMEM)],
        out_specs=pl.BlockSpec(memory_space=pl.ANY),
        scratch_shapes=[dma((1,)), dma((2 * n_seq,)), dma((n_seq,))],
        compiler_params=pltpu.CompilerParams(has_side_effects=True),
        name="gather_heads",
    )(chunk)


def return_kernel(n_seq, n_tp, blocks, terms, local_sem, send_sem, terms_sem):
    s, t = lax.axis_index("seq"), lax.axis_index("tp")
    half = n_seq // n_tp
    goal, slot = s // half, s % half
    go = Traffic(send_sem, (s, 1 - t))
    for d in range(1, n_seq):
        target = lax.rem(s + d, n_seq)
        go.send(blocks.at[target], terms.at[t, slot], terms_sem.at[t, slot], (target, goal))

    @pl.when(goal == t)
    def _():
        copy = pltpu.make_async_copy(blocks.at[s], terms.at[t, slot], local_sem.at[0])
        copy.start()
        copy.wait()

    @pl.when(goal != t)
    def _():
        copy = pltpu.make_async_remote_copy(
            src_ref=blocks.at[s],
            dst_ref=terms.at[t, slot],
            send_sem=send_sem.at[n_seq - 1],
            recv_sem=terms_sem.at[t, slot],
            device_id=(s, 1 - t),
            device_id_type=MESH,
        )
        copy.start()
        copy.wait_send()

    for part in range(n_tp):
        for k in range(half):
            owner = t * half + k

            @pl.when((owner != s) | (t != part))
            def _():
                go.arrive(terms.at[part, k], terms_sem.at[part, k])

    go.finish()


def return_blocks(blocks, n_seq, n_tp):
    dma = pltpu.SemaphoreType.DMA
    return pl.pallas_call(
        lambda *refs: return_kernel(n_seq, n_tp, *refs),
        out_shape=jax.ShapeDtypeStruct((n_tp, n_seq // n_tp) + blocks.shape[1:], blocks.dtype),
        in_specs=[pl.BlockSpec(memory_space=pltpu.VMEM)],
        out_specs=pl.BlockSpec(memory_space=pl.ANY),
        scratch_shapes=[dma((1,)), dma((n_seq,)), dma((n_tp, n_seq // n_tp))],
        compiler_params=pltpu.CompilerParams(has_side_effects=True),
        name="return_blocks",
    )(blocks)


def project_kernel(rows, wq, wkv, bias, cosine, sine, q_ref, k_ref, v_ref):
    spans, n_tp, span, width = rows.shape
    first, pair = bias[:, :HEAD_SIZE], bias[:, HEAD_SIZE:]
    query, both = first, pair
    for part in range(n_tp):
        piece = rows[:, part].reshape(spans * span, width)
        query = query + jnp.dot(
            piece, wq[pl.ds(part * width, width), :], preferred_element_type=jnp.float32
        )
        both = both + jnp.dot(
            piece, wkv[pl.ds(part * width, width), :], preferred_element_type=jnp.float32
        )

    def rotated(field):
        return (
            field * cosine[...] + pltpu.roll(field, HEAD_SIZE // 2, 1) * sine[...]
        ).astype(jnp.bfloat16)

    q_ref[...] = rotated(query)
    k_ref[...] = rotated(both[:, :HEAD_SIZE])
    v_ref[...] = both[:, HEAD_SIZE:].astype(jnp.bfloat16)


def project(rows, wq, wkv, bias, cosine, sine):
    n_seq, n_tp, span, width = rows.shape
    spans = math.gcd(n_seq, 4)
    table = pl.BlockSpec((spans * span, HEAD_SIZE), lambda i: (i, 0))
    whole = lambda a: pl.BlockSpec(a.shape, lambda i: (0, 0))
    out = jax.ShapeDtypeStruct((n_seq * span, HEAD_SIZE), jnp.bfloat16)
    return pl.pallas_call(
        project_kernel,
        grid=(n_seq // spans,),
        in_specs=[
            pl.BlockSpec((spans, n_tp, span, width), lambda i: (i, 0, 0, 0)),
            whole(wq),
            whole(wkv),
            whole(bias),
            table,
            table,
        ],
        out_specs=(table,) * 3,
        out_shape=(out,) * 3,
        name="project",
    )(rows, wq, wkv, bias, cosine, sine)


def per_device_by_head(
    hidden_in,
    span_order,
    norm_gain,
    w_query,
    bias_query,
    key_value_weight,
    bias_kv,
    w_out,
    post_gain,
):
    tok_rows, width = hidden_in.shape
    n_seq = span_order.shape[0]
    n_tp = MODEL_WIDTH // width
    me = lax.axis_index("seq")
    slab = w_query.shape[0]
    kv_heads = key_value_weight.shape[2] // HEAD_SIZE
    share = n_seq // kv_heads
    q_pieces = w_query.reshape(slab, n_seq, HEAD_SIZE).transpose(1, 0, 2)
    kv_pieces = (
        key_value_weight.reshape(slab, 2, kv_heads, HEAD_SIZE)
        .transpose(2, 0, 1, 3)
        .reshape(kv_heads, slab, 2 * HEAD_SIZE)
    )
    local = hidden_in.astype(jnp.float32)
    meansq = lax.psum(jnp.sum(local * local, axis=1, keepdims=True), "tp") / MODEL_WIDTH
    normed_in = (
        local * lax.rsqrt(meansq + eps) * norm_gain.astype(jnp.float32)[None, :]
    ).astype(jnp.bfloat16)
    rows, wq, wkv = exchange(normed_in, q_pieces, kv_pieces, n_seq, n_tp)
    bias_q = lax.dynamic_slice_in_dim(bias_query, me * HEAD_SIZE, HEAD_SIZE)
    bias_pair = lax.dynamic_slice_in_dim(bias_kv, me // share * HEAD_SIZE, HEAD_SIZE, 1)
    bias = jnp.concatenate([bias_q, bias_pair[0], bias_pair[1]]).astype(jnp.float32)
    positions, cosine, sine = rope_tables(span_order, tok_rows)
    queries, keys, values = project(
        rows,
        wq.reshape(n_seq * slab, HEAD_SIZE),
        wkv.reshape(n_seq * slab, 2 * HEAD_SIZE),
        bias[None, :],
        cosine,
        sine,
    )
    attended = attention(queries, keys, values, positions)
    heads = gather_heads(attended, n_seq)
    columns = w_out.shape[1]
    partial_out = jnp.einsum(
        "htd,hdc->tc",
        heads,
        w_out.reshape(n_seq, HEAD_SIZE, columns),
        preferred_element_type=jnp.float32,
    ).astype(jnp.bfloat16)
    terms = return_blocks(partial_out.reshape(n_seq, tok_rows, columns), n_seq, n_tp)
    mixed = jnp.sum(terms.astype(jnp.float32), axis=0).transpose(1, 0, 2).reshape(tok_rows, width)
    attn_out = mixed.astype(jnp.bfloat16)
    stream = local + mixed
    post_sq = lax.psum(jnp.sum(stream * stream, axis=1), "tp")
    normed = (
        stream
        * lax.rsqrt(post_sq / MODEL_WIDTH + eps)[:, None]
        * post_gain.astype(jnp.float32)[None, :]
    ).astype(jnp.bfloat16)
    return (attn_out, normed)


def per_device(*args):
    hidden_in, span_order, w_query, kv_weight = args[0], args[1], args[3], args[5]
    n_seq = span_order.shape[0]
    n_tp = MODEL_WIDTH // hidden_in.shape[1]
    heads = w_query.shape[1] // HEAD_SIZE
    kv_heads = kv_weight.shape[2] // HEAD_SIZE
    if n_tp == 2 and heads == n_seq and n_seq == kv_heads * GROUP and GROUP == PLANE:
        return per_device_by_head(*args)
    return per_device_by_span(*args)


def solution(mesh):
    placed = (
        P("seq", "tp"),
        P(),
        P("tp"),
        P("seq", "tp"),
        P("tp"),
        P("seq", None, "tp"),
        P(None, "tp"),
        P("tp", "seq"),
        P("tp"),
    )
    return jax.shard_map(
        per_device,
        mesh=mesh,
        in_specs=placed,
        out_specs=(P("seq", "tp"), P("seq", "tp")),
        check_vma=False,
    )
```

```python
import math

import jax
import jax.numpy as jnp
from jax import lax
from jax.experimental import pallas as pl
from jax.experimental.pallas import tpu as pltpu
from jax.sharding import PartitionSpec as P

MODEL_WIDTH = 4096
HEAD_SIZE = 128
GROUP = 4


eps = 1e-06
rope_base = 1000000.0


def apply_rotary(field, token_positions):
    half = field.shape[-1] // 2
    inverse = jnp.exp(-math.log(rope_base) * jnp.arange(half, dtype=jnp.float32) / half)
    angles = token_positions.astype(jnp.float32)[:, None] * inverse[None, :]
    cosine = jnp.cos(angles)[:, None, :]
    sine = jnp.sin(angles)[:, None, :]
    first = field[..., :half]
    second = field[..., half:]
    return jnp.concatenate(
        [first * cosine - second * sine, second * cosine + first * sine], axis=-1
    )


def span_lookup(order, devices):
    table_ids = jnp.arange(order.shape[0], dtype=jnp.int32)
    return jnp.sum(jnp.where(devices[:, None] == table_ids[None, :], order[None, :], 0), axis=1)


def per_device_by_span(
    hidden_in,
    span_order,
    norm_gain,
    w_query,
    bias_query,
    key_value_weight,
    bias_kv,
    w_out,
    post_gain,
):
    tok_rows = hidden_in.shape[0]
    seq_index = lax.axis_index("seq")
    own_span = span_lookup(span_order, jnp.full((1,), seq_index, jnp.int32))[0]
    token_positions = own_span * tok_rows + jnp.arange(tok_rows, dtype=jnp.int32)
    local = hidden_in.astype(jnp.float32)
    raw_rows, gains = (
        lax.all_gather(hidden_in, "tp", axis=1, tiled=True),
        lax.all_gather(norm_gain[None, :], "tp", axis=1, tiled=True),
    )
    full_rows = raw_rows.astype(jnp.float32)
    meansq = jnp.mean(full_rows * full_rows, axis=1, keepdims=True)
    normed_in = (full_rows * lax.rsqrt(meansq + eps) * gains.astype(jnp.float32)).astype(
        jnp.bfloat16
    )
    columns = normed_in
    query_proj = jnp.dot(
        columns,
        lax.all_gather(w_query, "seq", axis=0, tiled=True),
        preferred_element_type=jnp.float32,
    )
    columns = normed_in
    pair_proj = jnp.einsum(
        "tr,rkc->tkc",
        columns,
        lax.all_gather(key_value_weight, "seq", axis=0, tiled=True),
        preferred_element_type=jnp.float32,
    )
    query_heads = w_query.shape[1] // HEAD_SIZE
    kv_heads = key_value_weight.shape[2] // HEAD_SIZE
    query_proj = query_proj + bias_query.astype(jnp.float32)[None, :]
    queries = apply_rotary(
        query_proj.reshape(tok_rows, query_heads, HEAD_SIZE), token_positions
    ).astype(jnp.bfloat16)
    pair_proj = pair_proj + bias_kv.astype(jnp.float32)[None, :, :]
    rotated_keys = apply_rotary(
        pair_proj[:, 0, :].reshape(tok_rows, kv_heads, HEAD_SIZE), token_positions
    )
    rotated_keys = rotated_keys.astype(jnp.bfloat16).reshape(tok_rows, kv_heads * HEAD_SIZE)
    value_rows = pair_proj[:, 1, :].astype(jnp.bfloat16)
    grouped = (
        queries.reshape(tok_rows, kv_heads, GROUP, HEAD_SIZE)
        .transpose(1, 2, 0, 3)
        .reshape(kv_heads, GROUP * tok_rows, HEAD_SIZE)
    )
    query_pos = jnp.tile(token_positions, GROUP)
    last_query = jnp.max(token_positions)
    scale = 1.0 / math.sqrt(HEAD_SIZE)
    start_state = (
        jnp.full((kv_heads, GROUP * tok_rows), -1e30, jnp.float32),
        jnp.zeros((kv_heads, GROUP * tok_rows), jnp.float32),
        jnp.zeros((kv_heads, GROUP * tok_rows, HEAD_SIZE), jnp.float32),
    )
    key_piece = lax.all_gather(rotated_keys, "seq", axis=0, tiled=True)
    value_piece = lax.all_gather(value_rows, "seq", axis=0, tiled=True)
    count = key_piece.shape[0]
    block = math.gcd(count, 1536)

    def visit(step, state):
        first = step * block
        key_block = lax.dynamic_slice_in_dim(key_piece, first, block, 0).reshape(
            block, kv_heads, HEAD_SIZE
        )
        value_block = lax.dynamic_slice_in_dim(value_piece, first, block, 0).reshape(
            block, kv_heads, HEAD_SIZE
        )
        row_ids = first + jnp.arange(block, dtype=jnp.int32)
        key_pos = span_lookup(span_order, row_ids // tok_rows) * tok_rows + row_ids % tok_rows

        def update(current):
            maxima, totals, sums = current
            scores = (
                jnp.einsum("kqd,nkd->kqn", grouped, key_block, preferred_element_type=jnp.float32)
                * scale
            )
            allowed = (key_pos[None, :] <= query_pos[:, None])[None, :, :]
            scores = jnp.where(allowed, scores, -1e30)
            fresh = jnp.maximum(maxima, jnp.max(scores, axis=2))
            weights = jnp.where(allowed, jnp.exp(scores - fresh[:, :, None]), 0.0)
            factor = jnp.exp(maxima - fresh)
            totals = totals * factor + jnp.sum(weights, axis=2)
            sums = sums * factor[:, :, None] + jnp.einsum(
                "kqn,nkd->kqd",
                weights.astype(jnp.bfloat16),
                value_block,
                preferred_element_type=jnp.float32,
            )
            return (fresh, totals, sums)

        return lax.cond(jnp.min(key_pos) <= last_query, update, lambda current: current, state)

    maxima, totals, sums = lax.fori_loop(0, count // block, visit, start_state)
    attended = (sums / totals[:, :, None]).astype(jnp.bfloat16)
    attended = (
        attended.reshape(kv_heads, GROUP, tok_rows, HEAD_SIZE)
        .transpose(2, 0, 1, 3)
        .reshape(tok_rows, query_heads * HEAD_SIZE)
    )
    partial_out = jnp.dot(
        attended,
        lax.all_gather(w_out, "seq", axis=1, tiled=True),
        preferred_element_type=jnp.float32,
    )
    mixed = lax.psum_scatter(
        partial_out.astype(jnp.bfloat16), "tp", scatter_dimension=1, tiled=True
    ).astype(jnp.float32)
    attn_out = mixed.astype(jnp.bfloat16)
    stream = local + mixed
    post_sq = lax.psum(jnp.sum(stream * stream, axis=1), "tp")
    normed = (
        stream
        * lax.rsqrt(post_sq / MODEL_WIDTH + eps)[:, None]
        * post_gain.astype(jnp.float32)[None, :]
    ).astype(jnp.bfloat16)
    return (attn_out, normed)


def rope_tables(span_order, tok_rows):
    half = HEAD_SIZE // 2
    rows = (span_order[:, None] * tok_rows + jnp.arange(tok_rows, dtype=jnp.int32)[None, :]).reshape(-1)
    inverse = jnp.exp(-math.log(rope_base) * jnp.arange(half, dtype=jnp.float32) / half)
    angles = rows.astype(jnp.float32)[:, None] * inverse[None, :]
    cosine, sine = jnp.cos(angles), jnp.sin(angles)
    return (
        rows,
        jnp.concatenate([cosine, cosine], axis=1),
        jnp.concatenate([-sine, sine], axis=1),
    )


def attention_kernel(q_ref, k_ref, v_ref, qpos_ref, kpos_ref, out_ref):
    scores = lax.dot_general(
        q_ref[...], k_ref[...], (((1,), (1,)), ((), ())), preferred_element_type=jnp.float32
    ) * (1.0 / math.sqrt(HEAD_SIZE))
    allowed = kpos_ref[...] <= qpos_ref[...]
    scores = jnp.where(allowed, scores, -jnp.inf)
    peak = jnp.max(scores, axis=1, keepdims=True)
    weights = jnp.exp(scores - peak)
    totals = jnp.sum(weights, axis=1, keepdims=True)
    summed = jnp.dot(
        weights.astype(jnp.bfloat16), v_ref[...], preferred_element_type=jnp.float32
    )
    out_ref[...] = (summed / totals).astype(jnp.bfloat16)


def attention(queries, keys, values, positions):
    count = queries.shape[0]
    block = math.gcd(count, 256)
    rows = pl.BlockSpec((block, HEAD_SIZE), lambda i: (i, 0))
    whole = pl.BlockSpec((count, HEAD_SIZE), lambda i: (0, 0))
    return pl.pallas_call(
        attention_kernel,
        grid=(count // block,),
        in_specs=[
            rows,
            whole,
            whole,
            pl.BlockSpec((block, 1), lambda i: (i, 0)),
            pl.BlockSpec((1, count), lambda i: (0, 0)),
        ],
        out_specs=rows,
        out_shape=jax.ShapeDtypeStruct((count, HEAD_SIZE), jnp.bfloat16),
        cost_estimate=pl.CostEstimate(
            flops=4 * count * count * HEAD_SIZE,
            bytes_accessed=8 * count * HEAD_SIZE,
            transcendentals=count * count,
        ),
        name="attention",
    )(queries, keys, values, positions[:, None], positions[None, :])


MESH = pl.DeviceIdType.MESH
CORES = 2
PLANE = 4


class Traffic:
    def __init__(self, send_sem, peer):
        self.send_sem, self.peer, self.started = send_sem, peer, []

    def send(self, source, landing, arrival, target):
        copy = pltpu.make_async_remote_copy(
            src_ref=source,
            dst_ref=landing,
            send_sem=self.send_sem.at[len(self.started)],
            recv_sem=arrival,
            device_id=target,
            device_id_type=MESH,
        )
        copy.start()
        self.started.append(copy)

    def arrive(self, landing, arrival):
        pltpu.make_async_remote_copy(
            src_ref=landing,
            dst_ref=landing,
            send_sem=self.send_sem.at[0],
            recv_sem=arrival,
            device_id=self.peer,
            device_id_type=MESH,
        ).wait_recv()

    def finish(self):
        for copy in self.started:
            copy.wait_send()


def place(n_seq):
    s, t = lax.axis_index("seq"), lax.axis_index("tp")
    return s, t, s // PLANE, s % PLANE // CORES, s % CORES


def at(z, x, c):
    return z * PLANE + x * CORES + c


def exchange_kernel(
    n_seq, chunk, q_in, kv_in, rows_out, q_out, kv_out, local_sem, send_sem, rows_sem, q_sem, kv_sem
):
    s, t, z, x, c = place(n_seq)
    depth = n_seq // PLANE
    offset = s % PLANE
    sibling, across = (at(z, x, 1 - c), t), (at(z, 1 - x, c), t)
    other = (s, 1 - t)
    go = Traffic(send_sem, sibling)
    stay = [
        pltpu.make_async_copy(chunk, rows_out.at[s, t], local_sem.at[0]),
        pltpu.make_async_copy(q_in.at[s], q_out.at[s], local_sem.at[1]),
        pltpu.make_async_copy(kv_in.at[z], kv_out.at[s], local_sem.at[2]),
    ]
    for copy in stay:
        copy.start()

    def pass_on(source, owner, part, targets):
        for target in targets:
            go.send(source, rows_out.at[owner, part], rows_sem.at[owner, part], target)

    def await_rows(owner, part):
        go.arrive(rows_out.at[owner, part], rows_sem.at[owner, part])

    far = [lax.rem(z + d, depth) for d in range(1, depth)]
    near = [lax.rem(z - d + depth, depth) for d in range(depth)]
    pass_on(chunk, s, t, [other, across])
    pass_on(chunk, s, t, [(at(zt, x, c), t) for zt in far])
    pass_on(chunk, s, t, [sibling])
    for zt in far:
        target = at(zt, x, c)
        go.send(kv_in.at[zt], kv_out.at[s], kv_sem.at[s], (target, t))
    mates = [lax.rem(offset + r, PLANE) for r in range(1, PLANE)]
    for mate in mates:
        go.send(kv_in.at[z], kv_out.at[s], kv_sem.at[s], (z * PLANE + mate, t))
    for d in range(1, n_seq):
        target = lax.rem(s + d, n_seq)
        go.send(q_in.at[target], q_out.at[s], q_sem.at[s], (target, t))
    for zs in near[1:]:
        owner = at(zs, x, c)
        await_rows(owner, t)
        pass_on(rows_out.at[owner, t], owner, t, [other, across, sibling])
    for zs in near:
        owner = at(zs, 1 - x, c)
        await_rows(owner, t)
        pass_on(rows_out.at[owner, t], owner, t, [other, sibling])
    for zs in near[1:]:
        owner = at(zs, x, c)
        go.arrive(kv_out.at[owner], kv_sem.at[owner])
        for mate in mates:
            go.send(kv_out.at[owner], kv_out.at[owner], kv_sem.at[owner], (z * PLANE + mate, t))
    for xs in (x, 1 - x):
        for zs in near:
            owner = at(zs, xs, c)
            await_rows(owner, 1 - t)
            pass_on(rows_out.at[owner, 1 - t], owner, 1 - t, [sibling])
    for part in (t, 1 - t):
        for xs in (x, 1 - x):
            for zs in near:
                await_rows(at(zs, xs, 1 - c), part)
    for d in range(1, n_seq):
        owner = lax.rem(s - d + n_seq, n_seq)
        go.arrive(q_out.at[owner], q_sem.at[owner])
    for mate in mates:
        for zs in near:
            owner = zs * PLANE + mate
            go.arrive(kv_out.at[owner], kv_sem.at[owner])
    for copy in stay:
        copy.wait()
    go.finish()


def exchange(chunk, q_pieces, kv_pieces, n_seq, n_tp):
    vmem = pl.BlockSpec(memory_space=pltpu.VMEM)
    hbm = pl.BlockSpec(memory_space=pl.ANY)
    dma = pltpu.SemaphoreType.DMA
    return pl.pallas_call(
        lambda *refs: exchange_kernel(n_seq, *refs),
        out_shape=(
            jax.ShapeDtypeStruct((n_seq, n_tp) + chunk.shape, chunk.dtype),
            jax.ShapeDtypeStruct(q_pieces.shape, q_pieces.dtype),
            jax.ShapeDtypeStruct((n_seq,) + kv_pieces.shape[1:], kv_pieces.dtype),
        ),
        in_specs=[vmem] * 3,
        out_specs=(hbm,) * 3,
        scratch_shapes=[
            dma((3,)),
            dma((6 * n_seq,)),
            dma((n_seq, n_tp)),
            dma((n_seq,)),
            dma((n_seq,)),
        ],
        compiler_params=pltpu.CompilerParams(has_side_effects=True),
        cost_estimate=pl.CostEstimate(flops=0, bytes_accessed=16 * n_seq * n_tp * chunk.size, transcendentals=0),
        name="exchange",
    )(chunk, q_pieces, kv_pieces)


def heads_kernel(n_seq, chunk, heads_out, local_sem, send_sem, heads_sem):
    s, t, z, x, c = place(n_seq)
    depth = n_seq // PLANE
    sibling, across = (at(z, x, 1 - c), t), (at(z, 1 - x, c), t)
    go = Traffic(send_sem, sibling)
    stay = pltpu.make_async_copy(chunk.at[z], heads_out.at[s], local_sem.at[0])
    stay.start()
    near = [lax.rem(z - d + depth, depth) for d in range(depth)]
    for d in range(1, depth):
        zt = lax.rem(z + d, depth)
        go.send(chunk.at[zt], heads_out.at[s], heads_sem.at[s], (at(zt, x, c), t))
    for target in (across, sibling):
        go.send(chunk.at[z], heads_out.at[s], heads_sem.at[s], target)
    for zs in near[1:]:
        owner = at(zs, x, c)
        go.arrive(heads_out.at[owner], heads_sem.at[owner])
        for target in (across, sibling):
            go.send(heads_out.at[owner], heads_out.at[owner], heads_sem.at[owner], target)
    for zs in near:
        owner = at(zs, 1 - x, c)
        go.arrive(heads_out.at[owner], heads_sem.at[owner])
        go.send(heads_out.at[owner], heads_out.at[owner], heads_sem.at[owner], sibling)
    for xs in (x, 1 - x):
        for zs in near:
            owner = at(zs, xs, 1 - c)
            go.arrive(heads_out.at[owner], heads_sem.at[owner])
    stay.wait()
    go.finish()


def gather_heads(chunk, n_seq):
    dma = pltpu.SemaphoreType.DMA
    return pl.pallas_call(
        lambda *refs: heads_kernel(n_seq, *refs),
        out_shape=jax.ShapeDtypeStruct((n_seq,) + chunk.shape[1:], chunk.dtype),
        in_specs=[pl.BlockSpec(memory_space=pltpu.VMEM)],
        out_specs=pl.BlockSpec(memory_space=pl.ANY),
        scratch_shapes=[dma((1,)), dma((2 * n_seq,)), dma((n_seq,))],
        compiler_params=pltpu.CompilerParams(has_side_effects=True),
        name="gather_heads",
    )(chunk)


def mix_kernel(depth, heads, *refs):
    weights, out, flat = refs[:depth], refs[depth], refs[depth + 1]
    z = lax.axis_index("seq") // PLANE
    for head in range(heads.shape[0]):
        flat[:, head * HEAD_SIZE : (head + 1) * HEAD_SIZE] = heads[head]
    for d in range(depth):
        out[lax.rem(z - d + depth, depth)] = jnp.dot(
            flat[...], weights[d][...], preferred_element_type=jnp.float32
        ).astype(jnp.bfloat16)


def mix(heads, weights):
    n_heads, rows, size = heads.shape
    columns = weights[0].shape[1]
    vmem = pl.BlockSpec(memory_space=pltpu.VMEM)
    return pl.pallas_call(
        lambda *refs: mix_kernel(len(weights), *refs),
        out_shape=jax.ShapeDtypeStruct((len(weights), rows, columns), jnp.bfloat16),
        in_specs=[vmem] * (1 + len(weights)),
        out_specs=vmem,
        scratch_shapes=[pltpu.VMEM((rows, n_heads * size), jnp.bfloat16)],
        name="mix",
    )(heads, *weights)


def return_kernel(n_seq, n_tp, blocks, terms, local_sem, send_sem, terms_sem):
    s, t = lax.axis_index("seq"), lax.axis_index("tp")
    z, offset = s // PLANE, s % PLANE
    half = n_seq // PLANE // n_tp
    go = Traffic(send_sem, (s, 1 - t))

    def block(mate, goal):
        return blocks.at[pl.ds(goal * half, half), mate]

    pairs = [(r, q) for r in range(PLANE) for q in range(n_tp) if r or q]
    for r, q in pairs:
        mate, goal = lax.rem(offset + r, PLANE), lax.rem(t + q, n_tp)
        go.send(
            block(mate, goal), terms.at[t, offset], terms_sem.at[t, offset], (z * PLANE + mate, goal)
        )
    stay = pltpu.make_async_copy(block(offset, t), terms.at[t, offset], local_sem.at[0])
    stay.start()
    for r, q in pairs:
        mate, part = lax.rem(offset + r, PLANE), lax.rem(t + q, n_tp)
        go.arrive(terms.at[part, mate], terms_sem.at[part, mate])
    stay.wait()
    go.finish()


def return_blocks(blocks, n_seq, n_tp):
    dma = pltpu.SemaphoreType.DMA
    depth, mates, rows, columns = blocks.shape
    return pl.pallas_call(
        lambda *refs: return_kernel(n_seq, n_tp, *refs),
        out_shape=jax.ShapeDtypeStruct((n_tp, mates, depth // n_tp, rows, columns), blocks.dtype),
        in_specs=[pl.BlockSpec(memory_space=pltpu.VMEM)],
        out_specs=pl.BlockSpec(memory_space=pl.ANY),
        scratch_shapes=[dma((1,)), dma((n_tp * mates,)), dma((n_tp, mates))],
        compiler_params=pltpu.CompilerParams(has_side_effects=True),
        name="return_blocks",
    )(blocks)


def project_kernel(rows, wq, wkv, bias, cosine, sine, q_ref, k_ref, v_ref):
    spans, n_tp, span, width = rows.shape
    first, pair = bias[:, :HEAD_SIZE], bias[:, HEAD_SIZE:]
    query, both = first, pair
    for part in range(n_tp):
        piece = rows[:, part].reshape(spans * span, width)
        query = query + jnp.dot(
            piece, wq[pl.ds(part * width, width), :], preferred_element_type=jnp.float32
        )
        both = both + jnp.dot(
            piece, wkv[pl.ds(part * width, width), :], preferred_element_type=jnp.float32
        )

    def rotated(field):
        return (
            field * cosine[...] + pltpu.roll(field, HEAD_SIZE // 2, 1) * sine[...]
        ).astype(jnp.bfloat16)

    q_ref[...] = rotated(query)
    k_ref[...] = rotated(both[:, :HEAD_SIZE])
    v_ref[...] = both[:, HEAD_SIZE:].astype(jnp.bfloat16)


def project(rows, wq, wkv, bias, cosine, sine):
    n_seq, n_tp, span, width = rows.shape
    spans = math.gcd(n_seq, 4)
    table = pl.BlockSpec((spans * span, HEAD_SIZE), lambda i: (i, 0))
    whole = lambda a: pl.BlockSpec(a.shape, lambda i: (0, 0))
    out = jax.ShapeDtypeStruct((n_seq * span, HEAD_SIZE), jnp.bfloat16)
    return pl.pallas_call(
        project_kernel,
        grid=(n_seq // spans,),
        in_specs=[
            pl.BlockSpec((spans, n_tp, span, width), lambda i: (i, 0, 0, 0)),
            whole(wq),
            whole(wkv),
            whole(bias),
            table,
            table,
        ],
        out_specs=(table,) * 3,
        out_shape=(out,) * 3,
        cost_estimate=pl.CostEstimate(flops=6 * n_seq * n_tp * span * width * HEAD_SIZE, bytes_accessed=4 * rows.size, transcendentals=0),
        name="project",
    )(rows, wq, wkv, bias, cosine, sine)


def per_device_by_head(
    hidden_in,
    span_order,
    norm_gain,
    w_query,
    bias_query,
    key_value_weight,
    bias_kv,
    w_out,
    post_gain,
):
    tok_rows, width = hidden_in.shape
    n_seq = span_order.shape[0]
    n_tp = MODEL_WIDTH // width
    me = lax.axis_index("seq")
    slab = w_query.shape[0]
    kv_heads = key_value_weight.shape[2] // HEAD_SIZE
    share = n_seq // kv_heads
    depth = n_seq // PLANE
    out_weights = [w_out] + [
        lax.ppermute(w_out, "seq", [(i, (i + d * PLANE) % n_seq) for i in range(n_seq)])
        for d in range(1, depth)
    ]
    q_pieces = w_query.reshape(slab, n_seq, HEAD_SIZE).transpose(1, 0, 2)
    kv_pieces = (
        key_value_weight.reshape(slab, 2, kv_heads, HEAD_SIZE)
        .transpose(2, 0, 1, 3)
        .reshape(kv_heads, slab, 2 * HEAD_SIZE)
    )
    local = hidden_in.astype(jnp.float32)
    meansq = lax.psum(jnp.sum(local * local, axis=1, keepdims=True), "tp") / MODEL_WIDTH
    normed_in = (
        local * lax.rsqrt(meansq + eps) * norm_gain.astype(jnp.float32)[None, :]
    ).astype(jnp.bfloat16)
    rows, wq, wkv = exchange(normed_in, q_pieces, kv_pieces, n_seq, n_tp)
    bias_q = lax.dynamic_slice_in_dim(bias_query, me * HEAD_SIZE, HEAD_SIZE)
    bias_pair = lax.dynamic_slice_in_dim(bias_kv, me // share * HEAD_SIZE, HEAD_SIZE, 1)
    bias = jnp.concatenate([bias_q, bias_pair[0], bias_pair[1]]).astype(jnp.float32)
    positions, cosine, sine = rope_tables(span_order, tok_rows)
    queries, keys, values = project(
        rows,
        wq.reshape(n_seq * slab, HEAD_SIZE),
        wkv.reshape(n_seq * slab, 2 * HEAD_SIZE),
        bias[None, :],
        cosine,
        sine,
    )
    attended = attention(queries, keys, values, positions)
    heads = gather_heads(attended.reshape(depth, PLANE * tok_rows, HEAD_SIZE), n_seq)
    partial_out = mix(heads, out_weights)
    columns = w_out.shape[1]
    terms = return_blocks(partial_out.reshape(depth, PLANE, tok_rows, columns), n_seq, n_tp)
    mixed = jnp.sum(terms.astype(jnp.float32), axis=0).transpose(2, 1, 0, 3).reshape(tok_rows, width)
    attn_out = mixed.astype(jnp.bfloat16)
    stream = local + mixed
    post_sq = lax.psum(jnp.sum(stream * stream, axis=1), "tp")
    normed = (
        stream
        * lax.rsqrt(post_sq / MODEL_WIDTH + eps)[:, None]
        * post_gain.astype(jnp.float32)[None, :]
    ).astype(jnp.bfloat16)
    return (attn_out, normed)


def per_device(*args):
    hidden_in, span_order, w_query, kv_weight = args[0], args[1], args[3], args[5]
    n_seq = span_order.shape[0]
    n_tp = MODEL_WIDTH // hidden_in.shape[1]
    heads = w_query.shape[1] // HEAD_SIZE
    kv_heads = kv_weight.shape[2] // HEAD_SIZE
    if n_tp == 2 and heads == n_seq and n_seq == kv_heads * GROUP and GROUP == PLANE and n_seq % (PLANE * n_tp) == 0:
        return per_device_by_head(*args)
    return per_device_by_span(*args)


def solution(mesh):
    placed = (
        P("seq", "tp"),
        P(),
        P("tp"),
        P("seq", "tp"),
        P("tp"),
        P("seq", None, "tp"),
        P(None, "tp"),
        P("tp", "seq"),
        P("tp"),
    )
    return jax.shard_map(
        per_device,
        mesh=mesh,
        in_specs=placed,
        out_specs=(P("seq", "tp"), P("seq", "tp")),
        check_vma=False,
    )
```

```python
import math

import jax
import jax.numpy as jnp
from jax import lax
from jax.experimental import pallas as pl
from jax.experimental.pallas import tpu as pltpu
from jax.sharding import PartitionSpec as P

MODEL_WIDTH = 4096
HEAD_SIZE = 128
GROUP = 4


eps = 1e-06
rope_base = 1000000.0


def apply_rotary(field, token_positions):
    half = field.shape[-1] // 2
    inverse = jnp.exp(-math.log(rope_base) * jnp.arange(half, dtype=jnp.float32) / half)
    angles = token_positions.astype(jnp.float32)[:, None] * inverse[None, :]
    cosine = jnp.cos(angles)[:, None, :]
    sine = jnp.sin(angles)[:, None, :]
    first = field[..., :half]
    second = field[..., half:]
    return jnp.concatenate(
        [first * cosine - second * sine, second * cosine + first * sine], axis=-1
    )


def span_lookup(order, devices):
    table_ids = jnp.arange(order.shape[0], dtype=jnp.int32)
    return jnp.sum(jnp.where(devices[:, None] == table_ids[None, :], order[None, :], 0), axis=1)


def per_device_by_span(
    hidden_in,
    span_order,
    norm_gain,
    w_query,
    bias_query,
    key_value_weight,
    bias_kv,
    w_out,
    post_gain,
):
    tok_rows = hidden_in.shape[0]
    seq_index = lax.axis_index("seq")
    own_span = span_lookup(span_order, jnp.full((1,), seq_index, jnp.int32))[0]
    token_positions = own_span * tok_rows + jnp.arange(tok_rows, dtype=jnp.int32)
    local = hidden_in.astype(jnp.float32)
    raw_rows, gains = (
        lax.all_gather(hidden_in, "tp", axis=1, tiled=True),
        lax.all_gather(norm_gain[None, :], "tp", axis=1, tiled=True),
    )
    full_rows = raw_rows.astype(jnp.float32)
    meansq = jnp.mean(full_rows * full_rows, axis=1, keepdims=True)
    normed_in = (full_rows * lax.rsqrt(meansq + eps) * gains.astype(jnp.float32)).astype(
        jnp.bfloat16
    )
    columns = normed_in
    query_proj = jnp.dot(
        columns,
        lax.all_gather(w_query, "seq", axis=0, tiled=True),
        preferred_element_type=jnp.float32,
    )
    columns = normed_in
    pair_proj = jnp.einsum(
        "tr,rkc->tkc",
        columns,
        lax.all_gather(key_value_weight, "seq", axis=0, tiled=True),
        preferred_element_type=jnp.float32,
    )
    query_heads = w_query.shape[1] // HEAD_SIZE
    kv_heads = key_value_weight.shape[2] // HEAD_SIZE
    query_proj = query_proj + bias_query.astype(jnp.float32)[None, :]
    queries = apply_rotary(
        query_proj.reshape(tok_rows, query_heads, HEAD_SIZE), token_positions
    ).astype(jnp.bfloat16)
    pair_proj = pair_proj + bias_kv.astype(jnp.float32)[None, :, :]
    rotated_keys = apply_rotary(
        pair_proj[:, 0, :].reshape(tok_rows, kv_heads, HEAD_SIZE), token_positions
    )
    rotated_keys = rotated_keys.astype(jnp.bfloat16).reshape(tok_rows, kv_heads * HEAD_SIZE)
    value_rows = pair_proj[:, 1, :].astype(jnp.bfloat16)
    grouped = (
        queries.reshape(tok_rows, kv_heads, GROUP, HEAD_SIZE)
        .transpose(1, 2, 0, 3)
        .reshape(kv_heads, GROUP * tok_rows, HEAD_SIZE)
    )
    query_pos = jnp.tile(token_positions, GROUP)
    last_query = jnp.max(token_positions)
    scale = 1.0 / math.sqrt(HEAD_SIZE)
    start_state = (
        jnp.full((kv_heads, GROUP * tok_rows), -1e30, jnp.float32),
        jnp.zeros((kv_heads, GROUP * tok_rows), jnp.float32),
        jnp.zeros((kv_heads, GROUP * tok_rows, HEAD_SIZE), jnp.float32),
    )
    key_piece = lax.all_gather(rotated_keys, "seq", axis=0, tiled=True)
    value_piece = lax.all_gather(value_rows, "seq", axis=0, tiled=True)
    count = key_piece.shape[0]
    block = math.gcd(count, 1536)

    def visit(step, state):
        first = step * block
        key_block = lax.dynamic_slice_in_dim(key_piece, first, block, 0).reshape(
            block, kv_heads, HEAD_SIZE
        )
        value_block = lax.dynamic_slice_in_dim(value_piece, first, block, 0).reshape(
            block, kv_heads, HEAD_SIZE
        )
        row_ids = first + jnp.arange(block, dtype=jnp.int32)
        key_pos = span_lookup(span_order, row_ids // tok_rows) * tok_rows + row_ids % tok_rows

        def update(current):
            maxima, totals, sums = current
            scores = (
                jnp.einsum("kqd,nkd->kqn", grouped, key_block, preferred_element_type=jnp.float32)
                * scale
            )
            allowed = (key_pos[None, :] <= query_pos[:, None])[None, :, :]
            scores = jnp.where(allowed, scores, -1e30)
            fresh = jnp.maximum(maxima, jnp.max(scores, axis=2))
            weights = jnp.where(allowed, jnp.exp(scores - fresh[:, :, None]), 0.0)
            factor = jnp.exp(maxima - fresh)
            totals = totals * factor + jnp.sum(weights, axis=2)
            sums = sums * factor[:, :, None] + jnp.einsum(
                "kqn,nkd->kqd",
                weights.astype(jnp.bfloat16),
                value_block,
                preferred_element_type=jnp.float32,
            )
            return (fresh, totals, sums)

        return lax.cond(jnp.min(key_pos) <= last_query, update, lambda current: current, state)

    maxima, totals, sums = lax.fori_loop(0, count // block, visit, start_state)
    attended = (sums / totals[:, :, None]).astype(jnp.bfloat16)
    attended = (
        attended.reshape(kv_heads, GROUP, tok_rows, HEAD_SIZE)
        .transpose(2, 0, 1, 3)
        .reshape(tok_rows, query_heads * HEAD_SIZE)
    )
    partial_out = jnp.dot(
        attended,
        lax.all_gather(w_out, "seq", axis=1, tiled=True),
        preferred_element_type=jnp.float32,
    )
    mixed = lax.psum_scatter(
        partial_out.astype(jnp.bfloat16), "tp", scatter_dimension=1, tiled=True
    ).astype(jnp.float32)
    attn_out = mixed.astype(jnp.bfloat16)
    stream = local + mixed
    post_sq = lax.psum(jnp.sum(stream * stream, axis=1), "tp")
    normed = (
        stream
        * lax.rsqrt(post_sq / MODEL_WIDTH + eps)[:, None]
        * post_gain.astype(jnp.float32)[None, :]
    ).astype(jnp.bfloat16)
    return (attn_out, normed)


def rope_tables(span_order, tok_rows):
    half = HEAD_SIZE // 2
    rows = (span_order[:, None] * tok_rows + jnp.arange(tok_rows, dtype=jnp.int32)[None, :]).reshape(-1)
    inverse = jnp.exp(-math.log(rope_base) * jnp.arange(half, dtype=jnp.float32) / half)
    angles = rows.astype(jnp.float32)[:, None] * inverse[None, :]
    cosine, sine = jnp.cos(angles), jnp.sin(angles)
    return (
        rows,
        jnp.concatenate([cosine, cosine], axis=1),
        jnp.concatenate([-sine, sine], axis=1),
    )


def attention_kernel(q_ref, k_ref, v_ref, qpos_ref, kpos_ref, out_ref):
    scores = lax.dot_general(
        q_ref[...], k_ref[...], (((1,), (1,)), ((), ())), preferred_element_type=jnp.float32
    ) * (1.0 / math.sqrt(HEAD_SIZE))
    allowed = kpos_ref[...] <= qpos_ref[...]
    scores = jnp.where(allowed, scores, -jnp.inf)
    peak = jnp.max(scores, axis=1, keepdims=True)
    weights = jnp.exp(scores - peak)
    totals = jnp.sum(weights, axis=1, keepdims=True)
    summed = jnp.dot(
        weights.astype(jnp.bfloat16), v_ref[...], preferred_element_type=jnp.float32
    )
    out_ref[...] = (summed / totals).astype(jnp.bfloat16)


def attention(queries, keys, values, positions):
    count = queries.shape[0]
    block = math.gcd(count, 256)
    rows = pl.BlockSpec((block, HEAD_SIZE), lambda i: (i, 0))
    whole = pl.BlockSpec((count, HEAD_SIZE), lambda i: (0, 0))
    return pl.pallas_call(
        attention_kernel,
        grid=(count // block,),
        in_specs=[
            rows,
            whole,
            whole,
            pl.BlockSpec((block, 1), lambda i: (i, 0)),
            pl.BlockSpec((1, count), lambda i: (0, 0)),
        ],
        out_specs=rows,
        out_shape=jax.ShapeDtypeStruct((count, HEAD_SIZE), jnp.bfloat16),
        cost_estimate=pl.CostEstimate(
            flops=4 * count * count * HEAD_SIZE,
            bytes_accessed=8 * count * HEAD_SIZE,
            transcendentals=count * count,
        ),
        name="attention",
    )(queries, keys, values, positions[:, None], positions[None, :])


MESH = pl.DeviceIdType.MESH
CORES = 2
PLANE = 4


class Traffic:
    def __init__(self, send_sem, peer):
        self.send_sem, self.peer, self.started = send_sem, peer, []

    def send(self, source, landing, arrival, target):
        copy = pltpu.make_async_remote_copy(
            src_ref=source,
            dst_ref=landing,
            send_sem=self.send_sem.at[len(self.started)],
            recv_sem=arrival,
            device_id=target,
            device_id_type=MESH,
        )
        copy.start()
        self.started.append(copy)

    def arrive(self, landing, arrival):
        pltpu.make_async_remote_copy(
            src_ref=landing,
            dst_ref=landing,
            send_sem=self.send_sem.at[0],
            recv_sem=arrival,
            device_id=self.peer,
            device_id_type=MESH,
        ).wait_recv()

    def finish(self):
        for copy in self.started:
            copy.wait_send()


def place(n_seq):
    s, t = lax.axis_index("seq"), lax.axis_index("tp")
    return s, t, s // PLANE, s % PLANE // CORES, s % CORES


def at(z, x, c):
    return z * PLANE + x * CORES + c


def exchange_kernel(
    n_seq, chunk, q_in, kv_in, rows_out, q_out, kv_out, local_sem, send_sem, rows_sem, q_sem, kv_sem
):
    s, t, z, x, c = place(n_seq)
    depth = n_seq // PLANE
    offset = s % PLANE
    sibling, across = (at(z, x, 1 - c), t), (at(z, 1 - x, c), t)
    other = (s, 1 - t)
    go = Traffic(send_sem, sibling)
    stay = [
        pltpu.make_async_copy(chunk, rows_out.at[s, t], local_sem.at[0]),
        pltpu.make_async_copy(q_in.at[s], q_out.at[s], local_sem.at[1]),
        pltpu.make_async_copy(kv_in.at[z], kv_out.at[s], local_sem.at[2]),
    ]
    for copy in stay:
        copy.start()

    def pass_on(source, owner, part, targets):
        for target in targets:
            go.send(source, rows_out.at[owner, part], rows_sem.at[owner, part], target)

    def await_rows(owner, part):
        go.arrive(rows_out.at[owner, part], rows_sem.at[owner, part])

    far = [lax.rem(z + d, depth) for d in range(1, depth)]
    near = [lax.rem(z - d + depth, depth) for d in range(depth)]
    pass_on(chunk, s, t, [other, across])
    pass_on(chunk, s, t, [(at(zt, x, c), t) for zt in far])
    pass_on(chunk, s, t, [sibling])
    for zt in far:
        target = at(zt, x, c)
        go.send(kv_in.at[zt], kv_out.at[s], kv_sem.at[s], (target, t))
    mates = [lax.rem(offset + r, PLANE) for r in range(1, PLANE)]
    for mate in mates:
        go.send(kv_in.at[z], kv_out.at[s], kv_sem.at[s], (z * PLANE + mate, t))
    for d in range(1, n_seq):
        target = lax.rem(s + d, n_seq)
        go.send(q_in.at[target], q_out.at[s], q_sem.at[s], (target, t))
    for zs in near[1:]:
        owner = at(zs, x, c)
        await_rows(owner, t)
        pass_on(rows_out.at[owner, t], owner, t, [other, across, sibling])
    for zs in near:
        owner = at(zs, 1 - x, c)
        await_rows(owner, t)
        pass_on(rows_out.at[owner, t], owner, t, [other, sibling])
    for zs in near[1:]:
        owner = at(zs, x, c)
        go.arrive(kv_out.at[owner], kv_sem.at[owner])
        for mate in mates:
            go.send(kv_out.at[owner], kv_out.at[owner], kv_sem.at[owner], (z * PLANE + mate, t))
    for xs in (x, 1 - x):
        for zs in near:
            owner = at(zs, xs, c)
            await_rows(owner, 1 - t)
            pass_on(rows_out.at[owner, 1 - t], owner, 1 - t, [sibling])
    for part in (t, 1 - t):
        for xs in (x, 1 - x):
            for zs in near:
                await_rows(at(zs, xs, 1 - c), part)
    for d in range(1, n_seq):
        owner = lax.rem(s - d + n_seq, n_seq)
        go.arrive(q_out.at[owner], q_sem.at[owner])
    for mate in mates:
        for zs in near:
            owner = zs * PLANE + mate
            go.arrive(kv_out.at[owner], kv_sem.at[owner])
    for copy in stay:
        copy.wait()
    go.finish()


def exchange(chunk, q_pieces, kv_pieces, n_seq, n_tp):
    vmem = pl.BlockSpec(memory_space=pltpu.VMEM)
    hbm = pl.BlockSpec(memory_space=pl.ANY)
    dma = pltpu.SemaphoreType.DMA
    return pl.pallas_call(
        lambda *refs: exchange_kernel(n_seq, *refs),
        out_shape=(
            jax.ShapeDtypeStruct((n_seq, n_tp) + chunk.shape, chunk.dtype),
            jax.ShapeDtypeStruct(q_pieces.shape, q_pieces.dtype),
            jax.ShapeDtypeStruct((n_seq,) + kv_pieces.shape[1:], kv_pieces.dtype),
        ),
        in_specs=[vmem] * 3,
        out_specs=(hbm,) * 3,
        scratch_shapes=[
            dma((3,)),
            dma((6 * n_seq,)),
            dma((n_seq, n_tp)),
            dma((n_seq,)),
            dma((n_seq,)),
        ],
        compiler_params=pltpu.CompilerParams(has_side_effects=True),
        cost_estimate=pl.CostEstimate(flops=0, bytes_accessed=16 * n_seq * n_tp * chunk.size, transcendentals=0),
        name="exchange",
    )(chunk, q_pieces, kv_pieces)


def heads_kernel(n_seq, chunk, heads_out, local_sem, send_sem, heads_sem):
    s, t, z, x, c = place(n_seq)
    depth = n_seq // PLANE
    sibling, across = (at(z, x, 1 - c), t), (at(z, 1 - x, c), t)
    go = Traffic(send_sem, sibling)
    stay = pltpu.make_async_copy(chunk.at[z], heads_out.at[s], local_sem.at[0])
    stay.start()
    near = [lax.rem(z - d + depth, depth) for d in range(depth)]
    for d in range(1, depth):
        zt = lax.rem(z + d, depth)
        go.send(chunk.at[zt], heads_out.at[s], heads_sem.at[s], (at(zt, x, c), t))
    for target in (across, sibling):
        go.send(chunk.at[z], heads_out.at[s], heads_sem.at[s], target)
    for zs in near[1:]:
        owner = at(zs, x, c)
        go.arrive(heads_out.at[owner], heads_sem.at[owner])
        for target in (across, sibling):
            go.send(heads_out.at[owner], heads_out.at[owner], heads_sem.at[owner], target)
    for zs in near:
        owner = at(zs, 1 - x, c)
        go.arrive(heads_out.at[owner], heads_sem.at[owner])
        go.send(heads_out.at[owner], heads_out.at[owner], heads_sem.at[owner], sibling)
    for xs in (x, 1 - x):
        for zs in near:
            owner = at(zs, xs, 1 - c)
            go.arrive(heads_out.at[owner], heads_sem.at[owner])
    stay.wait()
    go.finish()


def gather_heads(chunk, n_seq):
    dma = pltpu.SemaphoreType.DMA
    return pl.pallas_call(
        lambda *refs: heads_kernel(n_seq, *refs),
        out_shape=jax.ShapeDtypeStruct((n_seq,) + chunk.shape[1:], chunk.dtype),
        in_specs=[pl.BlockSpec(memory_space=pltpu.VMEM)],
        out_specs=pl.BlockSpec(memory_space=pl.ANY),
        scratch_shapes=[dma((1,)), dma((2 * n_seq,)), dma((n_seq,))],
        compiler_params=pltpu.CompilerParams(has_side_effects=True),
        name="gather_heads",
    )(chunk)


def mix_kernel(depth, heads, *refs):
    weights, out, flat = refs[:depth], refs[depth], refs[depth + 1]
    z = lax.axis_index("seq") // PLANE
    for head in range(heads.shape[0]):
        flat[:, head * HEAD_SIZE : (head + 1) * HEAD_SIZE] = heads[head]
    for d in range(depth):
        out[lax.rem(z - d + depth, depth)] = jnp.dot(
            flat[...], weights[d][...], preferred_element_type=jnp.float32
        ).astype(jnp.bfloat16)


def mix(heads, weights):
    n_heads, rows, size = heads.shape
    columns = weights[0].shape[1]
    vmem = pl.BlockSpec(memory_space=pltpu.VMEM)
    return pl.pallas_call(
        lambda *refs: mix_kernel(len(weights), *refs),
        out_shape=jax.ShapeDtypeStruct((len(weights), rows, columns), jnp.bfloat16),
        in_specs=[vmem] * (1 + len(weights)),
        out_specs=vmem,
        scratch_shapes=[pltpu.VMEM((rows, n_heads * size), jnp.bfloat16)],
        name="mix",
    )(heads, *weights)


def return_kernel(n_seq, n_tp, blocks, terms, local_sem, send_sem, terms_sem):
    s, t = lax.axis_index("seq"), lax.axis_index("tp")
    z, offset = s // PLANE, s % PLANE
    half = n_seq // PLANE // n_tp
    go = Traffic(send_sem, (s, 1 - t))

    def block(mate, goal):
        return blocks.at[pl.ds(goal * half, half), mate]

    pairs = [(r, q) for r in range(PLANE) for q in range(n_tp) if r or q]
    for r, q in pairs:
        mate, goal = lax.rem(offset + r, PLANE), lax.rem(t + q, n_tp)
        go.send(
            block(mate, goal), terms.at[t, offset], terms_sem.at[t, offset], (z * PLANE + mate, goal)
        )
    stay = pltpu.make_async_copy(block(offset, t), terms.at[t, offset], local_sem.at[0])
    stay.start()
    for r, q in pairs:
        mate, part = lax.rem(offset + r, PLANE), lax.rem(t + q, n_tp)
        go.arrive(terms.at[part, mate], terms_sem.at[part, mate])
    stay.wait()
    go.finish()


def return_blocks(blocks, n_seq, n_tp):
    dma = pltpu.SemaphoreType.DMA
    depth, mates, rows, columns = blocks.shape
    return pl.pallas_call(
        lambda *refs: return_kernel(n_seq, n_tp, *refs),
        out_shape=jax.ShapeDtypeStruct((n_tp, mates, depth // n_tp, rows, columns), blocks.dtype),
        in_specs=[pl.BlockSpec(memory_space=pltpu.VMEM)],
        out_specs=pl.BlockSpec(memory_space=pl.ANY),
        scratch_shapes=[dma((1,)), dma((n_tp * mates,)), dma((n_tp, mates))],
        compiler_params=pltpu.CompilerParams(has_side_effects=True),
        name="return_blocks",
    )(blocks)


def project_kernel(rows, wq, wkv, bias, cosine, sine, q_ref, k_ref, v_ref):
    spans, n_tp, span, width = rows.shape
    first, pair = bias[:, :HEAD_SIZE], bias[:, HEAD_SIZE:]
    query, both = first, pair
    for part in range(n_tp):
        piece = rows[:, part].reshape(spans * span, width)
        query = query + jnp.dot(
            piece, wq[pl.ds(part * width, width), :], preferred_element_type=jnp.float32
        )
        both = both + jnp.dot(
            piece, wkv[pl.ds(part * width, width), :], preferred_element_type=jnp.float32
        )

    def rotated(field):
        return (
            field * cosine[...] + pltpu.roll(field, HEAD_SIZE // 2, 1) * sine[...]
        ).astype(jnp.bfloat16)

    q_ref[...] = rotated(query)
    k_ref[...] = rotated(both[:, :HEAD_SIZE])
    v_ref[...] = both[:, HEAD_SIZE:].astype(jnp.bfloat16)


def project(rows, wq, wkv, bias, cosine, sine):
    n_seq, n_tp, span, width = rows.shape
    spans = math.gcd(n_seq, 4)
    table = pl.BlockSpec((spans * span, HEAD_SIZE), lambda i: (i, 0))
    whole = lambda a: pl.BlockSpec(a.shape, lambda i: (0, 0))
    out = jax.ShapeDtypeStruct((n_seq * span, HEAD_SIZE), jnp.bfloat16)
    return pl.pallas_call(
        project_kernel,
        grid=(n_seq // spans,),
        in_specs=[
            pl.BlockSpec((spans, n_tp, span, width), lambda i: (i, 0, 0, 0)),
            whole(wq),
            whole(wkv),
            whole(bias),
            table,
            table,
        ],
        out_specs=(table,) * 3,
        out_shape=(out,) * 3,
        cost_estimate=pl.CostEstimate(flops=6 * n_seq * n_tp * span * width * HEAD_SIZE, bytes_accessed=4 * rows.size, transcendentals=0),
        name="project",
    )(rows, wq, wkv, bias, cosine, sine)


def per_device_by_head(
    hidden_in,
    span_order,
    norm_gain,
    w_query,
    bias_query,
    key_value_weight,
    bias_kv,
    w_out,
    post_gain,
):
    tok_rows, width = hidden_in.shape
    n_seq = span_order.shape[0]
    n_tp = MODEL_WIDTH // width
    me = lax.axis_index("seq")
    slab = w_query.shape[0]
    kv_heads = key_value_weight.shape[2] // HEAD_SIZE
    share = n_seq // kv_heads
    q_pieces = w_query.reshape(slab, n_seq, HEAD_SIZE).transpose(1, 0, 2)
    kv_pieces = (
        key_value_weight.reshape(slab, 2, kv_heads, HEAD_SIZE)
        .transpose(2, 0, 1, 3)
        .reshape(kv_heads, slab, 2 * HEAD_SIZE)
    )
    local = hidden_in.astype(jnp.float32)
    meansq = lax.psum(jnp.sum(local * local, axis=1, keepdims=True), "tp") / MODEL_WIDTH
    normed_in = (
        local * lax.rsqrt(meansq + eps) * norm_gain.astype(jnp.float32)[None, :]
    ).astype(jnp.bfloat16)
    rows, wq, wkv = exchange(normed_in, q_pieces, kv_pieces, n_seq, n_tp)
    rows, wq, wkv, w_out = lax.optimization_barrier((rows, wq, wkv, w_out))
    depth = n_seq // PLANE
    out_weights = [w_out] + [
        lax.ppermute(w_out, "seq", [(i, (i + d * PLANE) % n_seq) for i in range(n_seq)])
        for d in range(1, depth)
    ]
    bias_q = lax.dynamic_slice_in_dim(bias_query, me * HEAD_SIZE, HEAD_SIZE)
    bias_pair = lax.dynamic_slice_in_dim(bias_kv, me // share * HEAD_SIZE, HEAD_SIZE, 1)
    bias = jnp.concatenate([bias_q, bias_pair[0], bias_pair[1]]).astype(jnp.float32)
    positions, cosine, sine = rope_tables(span_order, tok_rows)
    queries, keys, values = project(
        rows,
        wq.reshape(n_seq * slab, HEAD_SIZE),
        wkv.reshape(n_seq * slab, 2 * HEAD_SIZE),
        bias[None, :],
        cosine,
        sine,
    )
    attended = attention(queries, keys, values, positions)
    heads = gather_heads(attended.reshape(depth, PLANE * tok_rows, HEAD_SIZE), n_seq)
    partial_out = mix(heads, out_weights)
    columns = w_out.shape[1]
    terms = return_blocks(partial_out.reshape(depth, PLANE, tok_rows, columns), n_seq, n_tp)
    mixed = jnp.sum(terms.astype(jnp.float32), axis=0).transpose(2, 1, 0, 3).reshape(tok_rows, width)
    attn_out = mixed.astype(jnp.bfloat16)
    stream = local + mixed
    post_sq = lax.psum(jnp.sum(stream * stream, axis=1), "tp")
    normed = (
        stream
        * lax.rsqrt(post_sq / MODEL_WIDTH + eps)[:, None]
        * post_gain.astype(jnp.float32)[None, :]
    ).astype(jnp.bfloat16)
    return (attn_out, normed)


def per_device(*args):
    hidden_in, span_order, w_query, kv_weight = args[0], args[1], args[3], args[5]
    n_seq = span_order.shape[0]
    n_tp = MODEL_WIDTH // hidden_in.shape[1]
    heads = w_query.shape[1] // HEAD_SIZE
    kv_heads = kv_weight.shape[2] // HEAD_SIZE
    if n_tp == 2 and heads == n_seq and n_seq == kv_heads * GROUP and GROUP == PLANE and n_seq % (PLANE * n_tp) == 0:
        return per_device_by_head(*args)
    return per_device_by_span(*args)


def solution(mesh):
    placed = (
        P("seq", "tp"),
        P(),
        P("tp"),
        P("seq", "tp"),
        P("tp"),
        P("seq", None, "tp"),
        P(None, "tp"),
        P("tp", "seq"),
        P("tp"),
    )
    return jax.shard_map(
        per_device,
        mesh=mesh,
        in_specs=placed,
        out_specs=(P("seq", "tp"), P("seq", "tp")),
        check_vma=False,
    )
```
